32 devices in a mesh: grp: 2 (over y), shard: 8 (over z, x), rep: 2 (over core).
Axes of the slice: x: 2, y: 2, z: 4, core: 2. Of those that a mesh axis runs over, the one named last changes fastest.
Arguments:
- replica_weights: bfloat16 [4, 4096, 14336], P(('grp', 'rep'), None, 'shard'), parts along dimension 0, may hold values from -6 to 6
- global_weights: float32 [8192, 14336], P(('grp', 'shard', 'rep')), parts along dimension 0, may hold values from -6 to 6
- momentum: float32 [8192, 14336], P(('grp', 'shard', 'rep')), parts along dimension 0, may hold values from -3 to 3
Outputs:
- new_params: bfloat16 [8192, 14336], P('grp', 'shard'), parts along dimension 0
- new_global: float32 [8192, 14336], P(('grp', 'shard', 'rep')), parts along dimension 0
- new_momentum: float32 [8192, 14336], P(('grp', 'shard', 'rep')), parts along dimension 0
The draws below stay inside these ranges and needn't reach their ends.
There are 2 independent parts, one for each index of `grp`. The reference program is written for one: setup_inputs(seed, part) draws one part's arguments, and reference() takes and returns one part's arrays. A program takes and returns all parts, laid end to end along the dimension named above; each array names one. Nothing has to cross between parts.
All inputs are finite; a program needn't handle non-finite values.
Results may differ from the reference program's by a relative error of at most 0.008.
Values may be sent and summed in bfloat16 or wider, within the bound.
A program may use at most 192 MiB of HBM per device.

```python
import jax
import jax.numpy as jnp

D = 4096
FF = 14336
REPLICAS = 2


def block_scale(rng, extent, pieces, smallest, top_value):
    loudness, own = 1.0, jax.random.fold_in(rng, 6)
    for position, parts in pieces:
        draws = jnp.exp(jax.random.uniform(jax.random.fold_in(own, position), (parts,), jnp.float32, smallest / len(pieces), top_value / len(pieces)))
        loudness = loudness * jnp.repeat(draws, extent[position] // parts).reshape([-1 if axis == position else 1 for axis in range(len(extent))])
    return loudness


def scatter_about(key, extent, spread, reach, cuts=(), dtype=jnp.bfloat16):
    array = jax.random.normal(key, extent, jnp.float32) * spread
    if len(cuts) > 0:
        array = block_scale(key, extent, cuts, -0.22, 0.18) * array
    return jnp.clip(array, min=-reach, max=reach).astype(dtype)


def setup_inputs(seed: int = 0, part: int = 0) -> dict:
    seeds = jax.random.split(jax.random.key(seed), 4)
    own_keys = jax.random.split(jax.random.fold_in(seeds[3], part), 4)
    replica_weights = scatter_about(own_keys[0], (REPLICAS, D, FF), 1.0, 6.0, ((0, 2), (2, 8)))
    global_weights = scatter_about(own_keys[1], (D, FF), 1.0, 6.0, ((0, 16),), jnp.float32)
    momentum = scatter_about(own_keys[2], (D, FF), 0.5, 3.0, ((0, 16),), jnp.float32)
    return dict(replica_weights=replica_weights, global_weights=global_weights, momentum=momentum)


outer_rate = 0.7
momentum_decay = 0.9


def reference(replica_weights, global_weights, momentum):
    total = jnp.sum(replica_weights.astype(jnp.float32), axis=0)
    delta = global_weights - total / jnp.float32(REPLICAS)
    new_momentum = momentum_decay * momentum + delta
    new_global = global_weights - outer_rate * (delta + momentum_decay * new_momentum)
    new_params = new_global.astype(jnp.bfloat16)
    return (new_params, new_global, new_momentum)
```

```python
import functools

import jax
import jax.numpy as jnp
from jax import lax
from jax.experimental import pallas as pl
from jax.experimental.pallas import tpu as pltpu
from jax.sharding import PartitionSpec as P

outer_rate = 0.7
momentum_decay = 0.9
LANES = 128
CHUNK = 16


def far_first(n):
    return sorted(range(1, n), key=lambda k: abs(2 * k - n)) + [0]


def exchange(n, pairs, w_ref, g_ref, m_ref, t_ref, p_ref, peer_w, tot, q_out, q_in,
             g_buf, m_buf, w_buf, load_g, load_m, load_w, w_send, w_recv,
             q_send, q_recv, t_send, t_recv, p_send, p_recv, p_local, t_local):
    me, rep = lax.axis_index("shard"), lax.axis_index("rep")
    other = 1 - rep
    owned, width = g_buf.shape[1:]
    steps = far_first(n)
    on_total = outer_rate * (1 + momentum_decay) / pairs
    on_global = 1 - outer_rate * (1 + momentum_decay)
    on_momentum = -outer_rate * momentum_decay * momentum_decay

    def ahead(k):
        return lax.rem(me + k, n)

    def columns(shard):
        return pl.ds(pl.multiple_of(shard * width, LANES), width)

    def rows(shard, which):
        return pl.ds(pl.multiple_of((shard * pairs + which) * owned, CHUNK), owned)

    def chunks(body):
        def one(j, carry):
            body(pl.ds(pl.multiple_of(j * CHUNK, CHUNK), CHUNK))
            return carry
        lax.fori_loop(0, owned // CHUNK, one, 0)

    def remote(src, dst, send, recv, to):
        return pltpu.make_async_remote_copy(
            src_ref=src, dst_ref=dst, send_sem=send, recv_sem=recv,
            device_id=to, device_id_type=pl.DeviceIdType.MESH)

    def outer_loads(i):
        cols = columns(ahead(steps[i]))
        return (pltpu.make_async_copy(g_ref.at[:, cols], g_buf.at[i % 2], load_g.at[i % 2]),
                pltpu.make_async_copy(m_ref.at[:, cols], m_buf.at[i % 2], load_m.at[i % 2]))

    def weight_load(i):
        return pltpu.make_async_copy(
            w_ref.at[rows(ahead(steps[i]), rep)], w_buf.at[i % 2], load_w.at[i % 2])

    for copy in outer_loads(0):
        copy.start()
    weight_load(0).start()

    barrier = pltpu.get_barrier_semaphore()
    for k in steps[:-1]:
        pl.semaphore_signal(barrier, inc=1, device_id={"shard": ahead(k)},
                            device_id_type=pl.DeviceIdType.MESH)
    pl.semaphore_signal(barrier, inc=1, device_id={"rep": other},
                        device_id_type=pl.DeviceIdType.MESH)
    pl.semaphore_wait(barrier, n)

    w_copies, q_copies, t_copies, p_copies, locals_ = [], [], [], [], []
    for i, k in enumerate(steps):
        copy = remote(w_ref.at[rows(ahead(k), other)], peer_w.at[i],
                      w_send.at[i], w_recv.at[i], {"rep": other})
        copy.start()
        w_copies.append(copy)

    for i, k in enumerate(steps):
        if i + 1 < n:
            for copy in outer_loads(i + 1):
                copy.start()
        for copy in outer_loads(i):
            copy.wait()
        out = q_out.at[i] if k else q_in.at[i]

        def state_term(at, i=i, out=out):
            out[at, :] = (on_global * g_buf[i % 2, at, :]
                          + on_momentum * m_buf[i % 2, at, :]).astype(out.dtype)
        chunks(state_term)
        if k:
            copy = remote(q_out.at[i], q_in.at[i], q_send.at[i], q_recv.at[i],
                          {"shard": ahead(k)})
            copy.start()
            q_copies.append(copy)

    for i, k in enumerate(steps):
        if i + 1 < n:
            weight_load(i + 1).start()
        weight_load(i).wait()
        w_copies[i].wait_recv()

        def add(at, i=i):
            tot[i, at, :] = (w_buf[i % 2, at, :].astype(jnp.float32)
                             + peer_w[i, at, :].astype(jnp.float32)).astype(tot.dtype)
        chunks(add)
        if k:
            copy = remote(tot.at[i], t_ref.at[:, columns(me)], t_send.at[i], t_recv.at[i],
                          {"shard": ahead(k)})
            t_copies.append(copy)
        else:
            copy = pltpu.make_async_copy(tot.at[i], t_ref.at[:, columns(me)], t_local)
            locals_.append(copy)
        copy.start()

    for j in [n - 1] + list(range(n - 1)):
        k = steps[j]
        i = steps.index((n - k) % n)
        if k:
            q_copies[j].wait_recv()

        def weights(at, i=i, j=j):
            q_in[j, at, :] = (q_in[j, at, :].astype(jnp.float32)
                              + on_total * tot[i, at, :].astype(jnp.float32)).astype(q_in.dtype)
        chunks(weights)
        target = p_ref.at[rows(ahead((n - k) % n), rep)]
        copy = remote(q_in.at[j], target, p_send.at[j], p_recv.at[j], {"rep": other})
        copy.start()
        p_copies.append(copy)
        copy = pltpu.make_async_copy(q_in.at[j], target, p_local.at[j])
        copy.start()
        locals_.append(copy)

    for copy in w_copies + q_copies:
        copy.wait_send()
    for copy in p_copies + t_copies:
        copy.wait()
    for copy in locals_:
        copy.wait()


def by_kernel(local, global_weights, momentum, n, pairs):
    owned = global_weights.shape[0]
    rows, width = local.shape
    anywhere = pl.BlockSpec(memory_space=pl.ANY)
    block = (owned, width)
    dma = pltpu.SemaphoreType.DMA
    return pl.pallas_call(
        functools.partial(exchange, n, pairs),
        out_shape=(jax.ShapeDtypeStruct((owned, n * width), jnp.bfloat16),
                   jax.ShapeDtypeStruct((rows, width), jnp.bfloat16)),
        in_specs=[anywhere] * 3,
        out_specs=(anywhere, anywhere),
        scratch_shapes=[pltpu.VMEM((n,) + block, jnp.bfloat16)] * 4
        + [pltpu.VMEM((2,) + block, jnp.float32)] * 2
        + [pltpu.VMEM((2,) + block, jnp.bfloat16)]
        + [dma((2,))] * 3 + [dma((n,))] * 9 + [dma],
        compiler_params=pltpu.CompilerParams(
            collective_id=0, has_side_effects=True, vmem_limit_bytes=60 * 2**20),
    )(local, global_weights, momentum)


def by_collectives(local, global_weights, momentum, n, pairs):
    owned = global_weights.shape[0]
    rows, width = local.shape
    halves = lax.psum_scatter(local.reshape(n, pairs, owned, width), "rep",
                              scatter_dimension=1, tiled=True).reshape(n * owned, width)
    total = lax.all_to_all(halves, "shard", split_axis=0, concat_axis=1, tiled=True)
    return total


def on_device(replica_weights, global_weights, momentum):
    local = replica_weights[0]
    rows, width = local.shape
    n, pairs = lax.axis_size("shard"), lax.axis_size("rep")
    owned = global_weights.shape[0]
    kernel = pairs == 2 and n > 1 and width % LANES == 0 and owned % CHUNK == 0
    whole = None
    if kernel:
        total, whole = by_kernel(local, global_weights, momentum, n, pairs)
    else:
        total = by_collectives(local, global_weights, momentum, n, pairs)
    delta = global_weights - total.astype(jnp.float32) / jnp.float32(pairs)
    new_momentum = momentum_decay * momentum + delta
    new_global = global_weights - outer_rate * (delta + momentum_decay * new_momentum)
    if not kernel:
        fresh = new_global.astype(jnp.bfloat16)
        spread = lax.all_to_all(fresh, "shard", split_axis=1, concat_axis=0, tiled=True)
        whole = lax.all_gather(
            spread.reshape(n, 1, owned, width), "rep", axis=1, tiled=True
        ).reshape(rows, width)
    return (whole, new_global, new_momentum)


def solution(mesh):
    placed = (
        P(("grp", "rep"), None, "shard"),
        P(("grp", "shard", "rep"), None),
        P(("grp", "shard", "rep"), None),
    )
    return jax.shard_map(
        on_device,
        mesh=mesh,
        in_specs=placed,
        out_specs=(
            P("grp", "shard"),
            P(("grp", "shard", "rep"), None),
            P(("grp", "shard", "rep"), None),
        ),
        check_vma=False,
    )
```

```python
import functools

import jax
import jax.numpy as jnp
from jax import lax
from jax.experimental import pallas as pl
from jax.experimental.pallas import tpu as pltpu
from jax.sharding import PartitionSpec as P

outer_rate = 0.7
momentum_decay = 0.9
LANES = 128
CHUNK = 16


def mixed(n):
    far = sorted(range(1, n), key=lambda k: abs(2 * k - n))
    return [far[j // 2] if j % 2 == 0 else far[-1 - j // 2] for j in range(n - 1)] + [0]


def exchange(n, pairs, w_ref, g_ref, m_ref, t_ref, p_ref, peer_w, tot, q_out, q_in,
             g_buf, m_buf, w_buf, load_g, load_m, load_w, w_send, w_recv,
             q_send, q_recv, t_send, t_recv, p_send, p_recv, p_local, t_local):
    me, rep = lax.axis_index("shard"), lax.axis_index("rep")
    other = 1 - rep
    owned, width = g_buf.shape[1:]
    steps = mixed(n)
    on_total = outer_rate * (1 + momentum_decay) / pairs
    on_global = 1 - outer_rate * (1 + momentum_decay)
    on_momentum = -outer_rate * momentum_decay * momentum_decay

    def ahead(k):
        return lax.rem(me + k, n)

    def columns(shard):
        return pl.ds(pl.multiple_of(shard * width, LANES), width)

    def rows(shard, which):
        return pl.ds(pl.multiple_of((shard * pairs + which) * owned, CHUNK), owned)

    def chunks(body):
        def one(j, carry):
            body(pl.ds(pl.multiple_of(j * CHUNK, CHUNK), CHUNK))
            return carry
        lax.fori_loop(0, owned // CHUNK, one, 0)

    def remote(src, dst, send, recv, to):
        return pltpu.make_async_remote_copy(
            src_ref=src, dst_ref=dst, send_sem=send, recv_sem=recv,
            device_id=to, device_id_type=pl.DeviceIdType.MESH)

    def outer_loads(i):
        cols = columns(ahead(steps[i]))
        return (pltpu.make_async_copy(g_ref.at[:, cols], g_buf.at[i % 2], load_g.at[i % 2]),
                pltpu.make_async_copy(m_ref.at[:, cols], m_buf.at[i % 2], load_m.at[i % 2]))

    def weight_load(i):
        return pltpu.make_async_copy(
            w_ref.at[rows(ahead(steps[i]), rep)], w_buf.at[i % 2], load_w.at[i % 2])

    for copy in outer_loads(0):
        copy.start()
    weight_load(0).start()

    barrier = pltpu.get_barrier_semaphore()
    for k in steps[:-1]:
        pl.semaphore_signal(barrier, inc=1, device_id={"shard": ahead(k)},
                            device_id_type=pl.DeviceIdType.MESH)
    pl.semaphore_signal(barrier, inc=1, device_id={"rep": other},
                        device_id_type=pl.DeviceIdType.MESH)
    pl.semaphore_wait(barrier, n)

    w_copies, q_copies, t_copies, p_copies, locals_ = [], [], [], [], []
    for i, k in enumerate(steps):
        copy = remote(w_ref.at[rows(ahead(k), other)], peer_w.at[i],
                      w_send.at[i], w_recv.at[i], {"rep": other})
        copy.start()
        w_copies.append(copy)

    for i, k in enumerate(steps):
        if i + 1 < n:
            for copy in outer_loads(i + 1):
                copy.start()
        for copy in outer_loads(i):
            copy.wait()
        out = q_out.at[i] if k else q_in.at[i]

        def state_term(at, i=i, out=out):
            out[at, :] = (on_global * g_buf[i % 2, at, :]
                          + on_momentum * m_buf[i % 2, at, :]).astype(out.dtype)
        chunks(state_term)
        if k:
            copy = remote(q_out.at[i], q_in.at[i], q_send.at[i], q_recv.at[i],
                          {"shard": ahead(k)})
            copy.start()
            q_copies.append(copy)

    for i, k in enumerate(steps):
        if i + 1 < n:
            weight_load(i + 1).start()
        weight_load(i).wait()
        w_copies[i].wait_recv()

        def add(at, i=i):
            tot[i, at, :] = (w_buf[i % 2, at, :].astype(jnp.float32)
                             + peer_w[i, at, :].astype(jnp.float32)).astype(tot.dtype)
        chunks(add)
        if k:
            copy = remote(tot.at[i], t_ref.at[:, columns(me)], t_send.at[i], t_recv.at[i],
                          {"shard": ahead(k)})
            t_copies.append(copy)
        else:
            copy = pltpu.make_async_copy(tot.at[i], t_ref.at[:, columns(me)], t_local)
            locals_.append(copy)
        copy.start()

    for j in [n - 1] + list(range(n - 1)):
        k = steps[j]
        i = steps.index((n - k) % n)
        if k:
            q_copies[j].wait_recv()

        def weights(at, i=i, j=j):
            q_in[j, at, :] = (q_in[j, at, :].astype(jnp.float32)
                              + on_total * tot[i, at, :].astype(jnp.float32)).astype(q_in.dtype)
        chunks(weights)
        target = p_ref.at[rows(ahead((n - k) % n), rep)]
        copy = remote(q_in.at[j], target, p_send.at[j], p_recv.at[j], {"rep": other})
        copy.start()
        p_copies.append(copy)
        copy = pltpu.make_async_copy(q_in.at[j], target, p_local.at[j])
        copy.start()
        locals_.append(copy)

    for copy in w_copies + q_copies:
        copy.wait_send()
    for copy in p_copies + t_copies:
        copy.wait()
    for copy in locals_:
        copy.wait()


def by_kernel(local, global_weights, momentum, n, pairs):
    owned = global_weights.shape[0]
    rows, width = local.shape
    anywhere = pl.BlockSpec(memory_space=pl.ANY)
    block = (owned, width)
    dma = pltpu.SemaphoreType.DMA
    return pl.pallas_call(
        functools.partial(exchange, n, pairs),
        out_shape=(jax.ShapeDtypeStruct((owned, n * width), jnp.bfloat16),
                   jax.ShapeDtypeStruct((rows, width), jnp.bfloat16)),
        in_specs=[anywhere] * 3,
        out_specs=(anywhere, anywhere),
        scratch_shapes=[pltpu.VMEM((n,) + block, jnp.bfloat16)] * 4
        + [pltpu.VMEM((2,) + block, jnp.float32)] * 2
        + [pltpu.VMEM((2,) + block, jnp.bfloat16)]
        + [dma((2,))] * 3 + [dma((n,))] * 9 + [dma],
        compiler_params=pltpu.CompilerParams(
            collective_id=0, has_side_effects=True, vmem_limit_bytes=60 * 2**20),
    )(local, global_weights, momentum)


def by_collectives(local, global_weights, momentum, n, pairs):
    owned = global_weights.shape[0]
    rows, width = local.shape
    halves = lax.psum_scatter(local.reshape(n, pairs, owned, width), "rep",
                              scatter_dimension=1, tiled=True).reshape(n * owned, width)
    total = lax.all_to_all(halves, "shard", split_axis=0, concat_axis=1, tiled=True)
    return total


def on_device(replica_weights, global_weights, momentum):
    local = replica_weights[0]
    rows, width = local.shape
    n, pairs = lax.axis_size("shard"), lax.axis_size("rep")
    owned = global_weights.shape[0]
    kernel = pairs == 2 and n > 1 and width % LANES == 0 and owned % CHUNK == 0
    whole = None
    if kernel:
        total, whole = by_kernel(local, global_weights, momentum, n, pairs)
    else:
        total = by_collectives(local, global_weights, momentum, n, pairs)
    delta = global_weights - total.astype(jnp.float32) / jnp.float32(pairs)
    new_momentum = momentum_decay * momentum + delta
    new_global = global_weights - outer_rate * (delta + momentum_decay * new_momentum)
    if not kernel:
        fresh = new_global.astype(jnp.bfloat16)
        spread = lax.all_to_all(fresh, "shard", split_axis=1, concat_axis=0, tiled=True)
        whole = lax.all_gather(
            spread.reshape(n, 1, owned, width), "rep", axis=1, tiled=True
        ).reshape(rows, width)
    return (whole, new_global, new_momentum)


def solution(mesh):
    placed = (
        P(("grp", "rep"), None, "shard"),
        P(("grp", "shard", "rep"), None),
        P(("grp", "shard", "rep"), None),
    )
    return jax.shard_map(
        on_device,
        mesh=mesh,
        in_specs=placed,
        out_specs=(
            P("grp", "shard"),
            P(("grp", "shard", "rep"), None),
            P(("grp", "shard", "rep"), None),
        ),
        check_vma=False,
    )
```
